32 devices in a mesh: grp: 4 (over z), elem: 8 (over y, x, core).
Axes of the slice: x: 2, y: 2, z: 4, core: 2. Of those that a mesh axis runs over, the one named last changes fastest.
Arguments:
- velocity: float32 [3, 343, 4096], P(None, None, ('grp', 'elem')), may hold values from -0.6 to 0.6
- adjoint: float32 [3, 343, 4096], P(None, None, ('grp', 'elem')), may hold values from -0.6 to 0.6
- spacing: float32 [3, 4096], P(None, ('grp', 'elem')), may hold values from 0.5 to 2
- elem_count: int32 [32], P(('grp', 'elem')), may hold values from 32 to 128, as said below
- design_map: int32 [8, 4096], P(None, ('grp', 'elem')), may hold values from 0 to 65535, as said below
Outputs:
- direction: float32 [3, 65536], P(None, ('grp', 'elem'))
- objective: float32 [], replicated
The draws below stay inside these ranges and needn't reach their ends.
Inputs may be any that keep to these rules, and one draw needn't show every extreme that they name: `elem_count`: the largest count equals 128 in every draw. `design_map`: design node d belongs to the device numbered d // 2048, counting grp first and elem second. Every entry of a device's columns names a node of a device whose elem index differs from that device's by at most one, cyclically over the elem axis, in any group.
All inputs are finite; a program needn't handle non-finite values.
Results may differ from the reference program's by a relative error of at most 0.0003.
Values sent between devices are 32-bit elements; how exact they have to be, the bound alone decides.
A program may use at most 64 MiB of HBM per device.

```python
import math
import jax
import jax.numpy as jnp
import numpy as np
from jax import lax

P_SIZE = 7
ELEM_DEV = 128
ND_DEV = 2048
ELEMS = 4096
N_GRP = 4
N_ELEM = 8


def node_field(key, salt):
    elements = ELEM_DEV * N_GRP * N_ELEM
    seeded = jax.random.fold_in(key, salt)
    jitter_key, shared_key = jax.random.split(seeded)
    shared_part = jnp.clip(jax.random.normal(shared_key, (3, P_SIZE ** 3, 1), jnp.float32), -4.0, 4.0)
    jitter_part = jnp.clip(jax.random.normal(jitter_key, (3, P_SIZE ** 3, elements), jnp.float32), -4.0, 4.0)
    return 0.07 * shared_part + 0.07 * jitter_part


def draw_velocity(key, part):
    return node_field(key, 11)


def draw_adjoint(key, part):
    return node_field(key, 23)


def draw_elem_count(key, part):
    devices = N_GRP * N_ELEM
    index = jnp.arange(devices, dtype=jnp.int32)
    base = ELEM_DEV // 3 + index * (ELEM_DEV - ELEM_DEV // 3) // (devices - 1)
    jitter = jax.random.randint(key, (devices,), 0, max(ELEM_DEV // 16, 2), dtype=jnp.int32)
    jitter = jnp.where(index == devices - 1, 0, jitter)
    return (base - jitter).astype(jnp.int32)


def draw_design_map(key, part):
    devices = N_GRP * N_ELEM
    total = ELEM_DEV * devices
    column = jnp.arange(total, dtype=jnp.int32)
    device = column // ELEM_DEV
    home_grp = (device // N_ELEM)[None, :]
    home_col = (device % N_ELEM)[None, :]
    first, second, third, fourth = jax.random.split(key, 4)
    same = jax.random.randint(first, (8, total), 0, 2, dtype=jnp.int32)
    other = jax.random.randint(second, (8, total), 1, N_GRP, dtype=jnp.int32)
    owner_grp = jnp.where(same == 1, home_grp, (home_grp + other) % N_GRP)
    offset = jax.random.randint(third, (8, total), -1, 2, dtype=jnp.int32)
    owner_col = (home_col + offset + N_ELEM) % N_ELEM
    vertex_ids = jnp.arange(8, dtype=jnp.int32)[:, None]
    within = 8 * jax.random.randint(fourth, (8, total), 0, ND_DEV // 8, dtype=jnp.int32) + vertex_ids
    return ((owner_grp * N_ELEM + owner_col) * ND_DEV + within).astype(jnp.int32)


def levels(stream_key, shape, cuts, low, top_value):
    factor_of = 1.0
    for position, blocks in cuts:
        draws = jax.random.uniform(jax.random.fold_in(jax.random.fold_in(stream_key, 6), position), (blocks,), jnp.float32, low / len(cuts), top_value / len(cuts))
        factor_of = factor_of * jnp.repeat(jnp.exp(draws), shape[position] // blocks).reshape((-1,) + (1,) * (len(shape) - 1 - position))
    return factor_of


def setup_inputs(seed: int = 0) -> dict:
    keys = jax.random.split(jax.random.key(seed), 6)
    velocity = draw_velocity(jax.random.fold_in(keys[5], 71), 0)
    adjoint = draw_adjoint(jax.random.fold_in(keys[5], 71), 0)
    spacing = jnp.clip(jnp.exp(math.log(2.0) - 1.3862944 * jax.random.uniform(keys[2], (3, ELEMS), jnp.float32) ** levels(keys[2], (3, ELEMS), ((1, 32),), -0.2, 0.2)), 0.5, 2.0)
    elem_count = draw_elem_count(jax.random.fold_in(keys[5], 71), 0)
    design_map = draw_design_map(jax.random.fold_in(keys[5], 71), 0)
    return {"velocity": velocity, "adjoint": adjoint, "spacing": spacing, "elem_count": elem_count, "design_map": design_map}


def lobatto(degree):
    points = np.cos(np.pi * np.arange(degree + 1) / degree)
    for sweep in range(60):
        lower = np.ones(degree + 1)
        upper = points.copy()
        for order in range(2, degree + 1):
            lower, upper = (upper, ((2 * order - 1) * points * upper - (order - 1) * lower) / order)
        points = points - (points * upper - lower) / ((degree + 1) * upper)
    lower = np.ones(degree + 1)
    upper = points.copy()
    for order in range(2, degree + 1):
        lower, upper = (upper, ((2 * order - 1) * points * upper - (order - 1) * lower) / order)
    return (points[::-1].copy(), upper[::-1].copy())

def tables():
    degree = P_SIZE - 1
    points, values = lobatto(degree)
    weights = 2.0 / (degree * (degree + 1) * values ** 2)
    derivative = np.zeros((P_SIZE, P_SIZE))
    for i in range(P_SIZE):
        for j in range(P_SIZE):
            if i != j:
                derivative[i, j] = values[i] / (values[j] * (points[i] - points[j]))
    derivative[0, 0] = -degree * (degree + 1) / 4.0
    derivative[P_SIZE - 1, P_SIZE - 1] = degree * (degree + 1) / 4.0
    coords = np.meshgrid(points, points, points, indexing='ij')
    coords = [c.reshape(-1) for c in coords]
    spread = np.meshgrid(weights, weights, weights, indexing='ij')
    quadrature = (spread[0] * spread[1] * spread[2]).reshape(-1)
    vertex_grad = np.zeros((3, 8, P_SIZE ** 3))
    for vertex in range(8):
        signs = [2.0 * (vertex >> 2 - m & 1) - 1.0 for m in range(3)]
        factors = [(1.0 + signs[m] * coords[m]) / 2.0 for m in range(3)]
        for j in range(3):
            others = [factors[m] for m in range(3) if m != j]
            vertex_grad[j, vertex] = signs[j] / 2.0 * others[0] * others[1] * quadrature
    return (jnp.asarray(derivative, jnp.float32), jnp.asarray(vertex_grad, jnp.float32), jnp.asarray(quadrature, jnp.float32))

def element_terms(velocity, adjoint, spacing, derivative, vertex_grad, quadrature):
    blocks = velocity.shape[-1]
    factor = 2.0 / spacing
    jacobian = spacing[0] * spacing[1] * spacing[2] / 8.0
    highest = lax.Precision.HIGHEST

    def gradient(field):
        cube = field.reshape(3, P_SIZE, P_SIZE, P_SIZE, blocks)
        first = jnp.einsum('ij,cjklb->ciklb', derivative, cube, precision=highest)
        second = jnp.einsum('ij,ckjlb->ckilb', derivative, cube, precision=highest)
        third = jnp.einsum('ij,ckljb->cklib', derivative, cube, precision=highest)
        stacked = jnp.stack([first, second, third], axis=1).reshape(3, 3, P_SIZE ** 3, blocks)
        return stacked * factor[None, :, None, :]
    grad_u = gradient(velocity)
    grad_w = gradient(adjoint)
    inner = lax.optimization_barrier(jnp.sum(grad_u * grad_w, axis=(0, 1)))
    cross = jnp.einsum('icqb,ijqb->cjqb', grad_u, grad_w, precision=highest)
    unit = jnp.eye(3, dtype=jnp.float32)
    stress = unit[:, :, None, None] * inner[None, None] - cross - jnp.swapaxes(cross, 0, 1)
    contrib = jnp.einsum('cjqb,jkq->cjkb', stress, vertex_grad, precision=highest)
    terms = lax.optimization_barrier(jnp.sum(contrib * factor[None, :, None, :], axis=1)) * jacobian[None, None, :]
    squared = lax.optimization_barrier(jnp.sum(grad_u * grad_u, axis=(0, 1)))
    dissipated = jacobian * jnp.einsum('qb,q->b', squared, quadrature, precision=highest)
    return (terms, dissipated)

def reference(velocity, adjoint, spacing, elem_count, design_map):
    devices = N_GRP * N_ELEM
    design_total = ND_DEV * devices
    derivative, vertex_grad, quadrature = tables()

    def one_device(carry, device):
        gradient_sum, spent = carry
        start = (device * ELEM_DEV).astype(jnp.int32)
        field_u = lax.dynamic_slice_in_dim(velocity, start, ELEM_DEV, 2)
        field_w = lax.dynamic_slice_in_dim(adjoint, start, ELEM_DEV, 2)
        lengths = lax.dynamic_slice_in_dim(spacing, start, ELEM_DEV, 1)
        nodes = lax.dynamic_slice_in_dim(design_map, start, ELEM_DEV, 1)
        terms, dissipated = element_terms(field_u, field_w, lengths, derivative, vertex_grad, quadrature)
        live = (jnp.arange(ELEM_DEV, dtype=jnp.int32) < elem_count[device]).astype(jnp.float32)
        terms = terms * live[None, None, :]
        gradient_sum = gradient_sum.at[:, nodes.reshape(-1)].add(terms.reshape(3, -1))
        return ((gradient_sum, spent + jnp.sum(dissipated * live)), None)
    init = (jnp.zeros((3, design_total), jnp.float32), jnp.zeros((), jnp.float32))
    (gradient_sum, spent), _ = lax.scan(one_device, init, jnp.arange(devices, dtype=jnp.int32))
    mean_square = jnp.sum(gradient_sum * gradient_sum) / (3.0 * design_total)
    direction = gradient_sum * lax.rsqrt(mean_square + 1e-06)
    objective = spent / (P_SIZE ** 3 * ELEM_DEV * devices)
    return (direction, objective)
```

```python
import functools

import jax
import jax.numpy as jnp
import numpy as np
from jax import lax
from jax.experimental import pallas as pl
from jax.experimental.pallas import tpu as pltpu
from jax.sharding import PartitionSpec as P

P_SIZE = 7
ND_DEV = 2048
LANES = 128
LOW = 256
NODES = P_SIZE**3
ROWS = -(-NODES // 16) * 16
MESH = pl.DeviceIdType.MESH
F32 = jnp.float32
BF16 = jnp.bfloat16


def lobatto(degree):
    points = np.cos(np.pi * np.arange(degree + 1) / degree)
    for sweep in range(60):
        lower = np.ones(degree + 1)
        upper = points.copy()
        for order in range(2, degree + 1):
            lower, upper = (upper, ((2 * order - 1) * points * upper - (order - 1) * lower) / order)
        points = points - (points * upper - lower) / ((degree + 1) * upper)
    lower = np.ones(degree + 1)
    upper = points.copy()
    for order in range(2, degree + 1):
        lower, upper = (upper, ((2 * order - 1) * points * upper - (order - 1) * lower) / order)
    return (points[::-1].copy(), upper[::-1].copy())


def halves(table):
    exact = np.asarray(table, np.float32)
    high = exact.astype(BF16)
    low = (exact - high.astype(np.float32)).astype(BF16)
    return (high, low)


def tables():
    degree = P_SIZE - 1
    points, values = lobatto(degree)
    weights = 2.0 / (degree * (degree + 1) * values**2)
    derivative = np.zeros((P_SIZE, P_SIZE))
    for i in range(P_SIZE):
        for j in range(P_SIZE):
            if i != j:
                derivative[i, j] = values[i] / (values[j] * (points[i] - points[j]))
    derivative[0, 0] = -degree * (degree + 1) / 4.0
    derivative[P_SIZE - 1, P_SIZE - 1] = degree * (degree + 1) / 4.0
    coords = np.meshgrid(points, points, points, indexing="ij")
    coords = [c.reshape(-1) for c in coords]
    spread = np.meshgrid(weights, weights, weights, indexing="ij")
    quadrature = (spread[0] * spread[1] * spread[2]).reshape(-1)
    contract = np.zeros((32, ROWS))
    for vertex in range(8):
        signs = [2.0 * (vertex >> 2 - m & 1) - 1.0 for m in range(3)]
        factors = [(1.0 + signs[m] * coords[m]) / 2.0 for m in range(3)]
        for j in range(3):
            others = [factors[m] for m in range(3) if m != j]
            contract[8 * j + vertex, :NODES] = signs[j] / 2.0 * others[0] * others[1] * quadrature
    contract[24, :NODES] = quadrature
    unit = np.eye(P_SIZE)
    directional = np.zeros((3, ROWS, NODES))
    directional[0, :NODES] = np.kron(np.kron(derivative, unit), unit)
    directional[1, :NODES] = np.kron(np.kron(unit, derivative), unit)
    directional[2, :NODES] = np.kron(np.kron(unit, unit), derivative)
    return (
        *halves(directional.reshape(3 * ROWS, NODES)),
        np.concatenate(halves(contract)),
    )


def split(value):
    high = value.astype(BF16)
    return (high, (value - high.astype(F32)).astype(BF16))


def quotient(value, by):
    if by & (by - 1) == 0:
        return lax.shift_right_logical(value, jnp.full_like(value, by.bit_length() - 1))
    return lax.div(value, jnp.full_like(value, by))


def remainder(value, by):
    if by & (by - 1) == 0:
        return value & (by - 1)
    return lax.rem(value, jnp.full_like(value, by))


def element_terms(fields, spacing, live, high, low, contract):
    slots = spacing.shape[1]
    field_high, field_low = split(fields)
    grads = (
        jnp.dot(high, field_high, preferred_element_type=F32)
        + jnp.dot(low, field_high, preferred_element_type=F32)
        + jnp.dot(high, field_low, preferred_element_type=F32)
    )

    def grad(field, i, j):
        column = (3 * field + i) * slots
        return grads[j * ROWS : (j + 1) * ROWS, column : column + slots]

    def product(c, j):
        return sum(grad(0, i, c) * grad(1, i, j) for i in range(3))

    pairs = [(0, 1), (0, 2), (1, 2)]
    stack = [product(m, m) for m in range(3)]
    stack += [product(c, j) + product(j, c) for c, j in pairs]
    stack += [sum(grad(0, i, j) * grad(0, i, j) for i in range(3)) for j in range(3)]
    stack_high, stack_low = split(jnp.concatenate(stack, axis=1))
    both = jnp.dot(contract, stack_high, preferred_element_type=F32)
    sums = both[:32] + both[32:] + jnp.dot(contract[:32], stack_low, preferred_element_type=F32)

    def part(j, column):
        return sums[8 * j : 8 * j + 8, column * slots : (column + 1) * slots]

    factor = [2.0 / spacing[j : j + 1] for j in range(3)]
    square = [f * f for f in factor]
    jacobian = spacing[0:1] * spacing[1:2] * spacing[2:3] * 0.125
    terms = []
    for c in range(3):
        total = sum(square[m] * part(c, m) for m in range(3)) - 2.0 * square[c] * part(c, c)
        for column, pair in enumerate(pairs):
            if c in pair:
                j = pair[0] + pair[1] - c
                total = total - square[j] * part(j, 3 + column)
        terms.append(jnp.where(live, total * (factor[c] * jacobian), 0.0))
    spent = sum(square[j] * part(3, 6 + j) for j in range(3)) * jacobian
    return (terms, jnp.where(live, spent, 0.0))


def assemble(terms, target, blocks):
    upper = quotient(target, LOW)
    lower = remainder(target, LOW)
    slots = target.shape[1]
    rows = blocks * (ND_DEV // LOW)
    row_index = lax.broadcasted_iota(jnp.int32, (rows, slots), 0)
    low_index = lax.broadcasted_iota(jnp.int32, (LOW, slots), 0)
    parts = []
    for term in terms:
        high = term.astype(BF16).astype(F32)
        parts.append(high)
    for c in range(3):
        parts.append(terms[c] - parts[c])
    left = []
    right = []
    for k in range(8):
        hit = row_index == upper[k : k + 1]
        left.append(
            jnp.concatenate([jnp.where(hit, p[k : k + 1], 0.0).astype(BF16) for p in parts], axis=0)
        )
        right.append(jnp.where(low_index == lower[k : k + 1], 1.0, 0.0).astype(BF16))
    sums = lax.dot_general(
        jnp.concatenate(left, axis=1),
        jnp.concatenate(right, axis=1),
        (((1,), (1,)), ((), ())),
        preferred_element_type=F32,
    )
    return [sums[c * rows : (c + 1) * rows] + sums[(3 + c) * rows : (4 + c) * rows] for c in range(3)]


def kernel(
    groups, columns,
    velocity, adjoint, spacing, count, design_map, high, low, contract,
    direction, objective,
    outgoing, arrived, gathered, send_sem, recv_sem, send_all, recv_all,
):
    devices = groups * columns
    grp, col = lax.axis_index("grp"), lax.axis_index("elem")
    me = grp * columns + col
    slots = spacing.shape[1]

    barrier = pltpu.get_barrier_semaphore()

    def coords(step):
        peer = lax.rem(me + step, devices)
        return (peer // columns, lax.rem(peer, columns))

    def greet(step, carry):
        pl.semaphore_signal(barrier, inc=1, device_id=coords(step), device_id_type=MESH)
        return carry

    lax.fori_loop(1, devices, greet, 0)

    live = lax.broadcasted_iota(jnp.int32, (8, slots), 1) < count[0]
    fields = jnp.concatenate([f[i] for f in (velocity, adjoint) for i in range(3)], axis=1)
    terms, spent = element_terms(fields, spacing[...], live, high[...], low[...], contract[...])
    node = design_map[...]
    owner = quotient(node, ND_DEV)
    offset = remainder(remainder(owner, columns) - col + (1 + columns), columns)
    block = offset * groups + quotient(owner, columns)
    sums = assemble(terms, block * ND_DEV + remainder(node, ND_DEV), 3 * groups)
    for b in range(3 * groups):
        for c in range(3):
            outgoing[b, 8 * c : 8 * c + 8, :] = sums[c][8 * b : 8 * b + 8]

    pl.semaphore_wait(barrier, devices - 1)

    copies = []
    for step in [*range(groups // 2, groups), *range(groups // 2)]:
        for o in range(3):
            if step == 0 and o == 1:
                continue
            to_grp = lax.rem(grp + step, groups)
            slot = o * groups + step
            copy = pltpu.make_async_remote_copy(
                src_ref=outgoing.at[o * groups + to_grp],
                dst_ref=arrived.at[slot],
                send_sem=send_sem.at[slot],
                recv_sem=recv_sem.at[slot],
                device_id=(to_grp, lax.rem(col + (o - 1 + columns), columns)),
                device_id_type=MESH,
            )
            copy.start()
            copies.append((slot, copy))
    total = outgoing[groups + grp]
    for slot, copy in copies[::-1]:
        copy.wait_recv()
        total = total + arrived[slot]

    squares = total * total
    squares = squares[0:8] + squares[8:16] + squares[16:24]
    squares = squares[:, :LANES] + squares[:, LANES:]
    lane = lax.broadcasted_iota(jnp.int32, (8, LANES), 1)
    mixed = jnp.where(
        lane < LANES // 2,
        squares + pltpu.roll(squares, LANES // 2, 1),
        spent + pltpu.roll(spent, LANES // 2, 1),
    )
    gathered[me] = jnp.sum(mixed, axis=0, keepdims=True)

    def share(step):
        return pltpu.make_async_remote_copy(
            src_ref=gathered.at[me],
            dst_ref=gathered.at[me],
            send_sem=send_all.at[step],
            recv_sem=recv_all.at[step],
            device_id=coords(step),
            device_id_type=MESH,
        )

    def send(step, carry):
        share(step).start()
        return carry

    def receive(step, carry):
        share(step).wait_recv()
        return carry

    def finish(step, carry):
        share(step).wait_send()
        return carry

    lax.fori_loop(1, devices, send, 0)
    for slot, copy in copies:
        copy.wait_send()
    lax.fori_loop(1, devices, receive, 0)
    everything = jnp.sum(gathered[...], axis=0)
    first = lax.broadcasted_iota(jnp.int32, (1, LANES), 1) < LANES // 2
    square_total = jnp.sum(jnp.where(first, everything, 0.0), axis=1, keepdims=True)
    spent_total = jnp.sum(jnp.where(first, 0.0, everything), axis=1, keepdims=True)
    scale = lax.rsqrt(square_total * (1.0 / (3.0 * ND_DEV * devices)) + 1e-06)
    scaled = total * scale
    for c in range(3):
        direction[c] = scaled[8 * c : 8 * c + 8]
    objective[...] = spent_total * (1.0 / (NODES * slots * devices))
    lax.fori_loop(1, devices, finish, 0)


def body(groups, columns, velocity, adjoint, spacing, elem_count, design_map):
    devices = groups * columns
    blocks = 3 * groups
    vmem = pl.BlockSpec(memory_space=pltpu.VMEM)
    direction, objective = pl.pallas_call(
        functools.partial(kernel, groups, columns),
        out_shape=(
            jax.ShapeDtypeStruct((3, ND_DEV // LOW, LOW), F32),
            jax.ShapeDtypeStruct((1, 1), F32),
        ),
        in_specs=[vmem, vmem, vmem, pl.BlockSpec(memory_space=pltpu.SMEM), vmem, vmem, vmem, vmem],
        out_specs=(vmem, vmem),
        scratch_shapes=[
            pltpu.VMEM((blocks, 24, LOW), F32),
            pltpu.VMEM((blocks, 24, LOW), F32),
            pltpu.VMEM((devices, 1, LANES), F32),
            pltpu.SemaphoreType.DMA((blocks,)),
            pltpu.SemaphoreType.DMA((blocks,)),
            pltpu.SemaphoreType.DMA((devices,)),
            pltpu.SemaphoreType.DMA((devices,)),
        ],
        compiler_params=pltpu.CompilerParams(collective_id=0, has_side_effects=True),
    )(velocity, adjoint, spacing, elem_count, design_map, *tables())
    return (direction.reshape(3, ND_DEV), objective.reshape(()))


def solution(mesh):
    return jax.shard_map(
        functools.partial(body, mesh.shape["grp"], mesh.shape["elem"]),
        mesh=mesh,
        in_specs=(
            P(None, None, ("grp", "elem")),
            P(None, None, ("grp", "elem")),
            P(None, ("grp", "elem")),
            P(("grp", "elem")),
            P(None, ("grp", "elem")),
        ),
        out_specs=(P(None, ("grp", "elem")), P()),
        check_vma=False,
    )
```

```python
import functools

import jax
import jax.numpy as jnp
import numpy as np
from jax import lax
from jax.experimental import pallas as pl
from jax.experimental.pallas import tpu as pltpu
from jax.sharding import PartitionSpec as P

P_SIZE = 7
ND_DEV = 2048
LANES = 128
UPPER = ND_DEV // LANES
NODES = P_SIZE**3
ROWS = -(-NODES // 16) * 16
HEAD = 240
BACK = 192
TAIL = ROWS - HEAD
MESH = pl.DeviceIdType.MESH
F32 = jnp.float32
BF16 = jnp.bfloat16


def lobatto(degree):
    points = np.cos(np.pi * np.arange(degree + 1) / degree)
    for sweep in range(60):
        lower = np.ones(degree + 1)
        upper = points.copy()
        for order in range(2, degree + 1):
            lower, upper = (upper, ((2 * order - 1) * points * upper - (order - 1) * lower) / order)
        points = points - (points * upper - lower) / ((degree + 1) * upper)
    lower = np.ones(degree + 1)
    upper = points.copy()
    for order in range(2, degree + 1):
        lower, upper = (upper, ((2 * order - 1) * points * upper - (order - 1) * lower) / order)
    return (points[::-1].copy(), upper[::-1].copy())


def halves(table):
    exact = np.asarray(table, np.float32)
    high = exact.astype(BF16)
    low = (exact - high.astype(np.float32)).astype(BF16)
    return (high, low)


def tables():
    degree = P_SIZE - 1
    points, values = lobatto(degree)
    weights = 2.0 / (degree * (degree + 1) * values**2)
    derivative = np.zeros((P_SIZE, P_SIZE))
    for i in range(P_SIZE):
        for j in range(P_SIZE):
            if i != j:
                derivative[i, j] = values[i] / (values[j] * (points[i] - points[j]))
    derivative[0, 0] = -degree * (degree + 1) / 4.0
    derivative[P_SIZE - 1, P_SIZE - 1] = degree * (degree + 1) / 4.0
    coords = np.meshgrid(points, points, points, indexing="ij")
    coords = [c.reshape(-1) for c in coords]
    spread = np.meshgrid(weights, weights, weights, indexing="ij")
    quadrature = (spread[0] * spread[1] * spread[2]).reshape(-1)
    contract = np.zeros((32, ROWS))
    for vertex in range(8):
        signs = [2.0 * (vertex >> 2 - m & 1) - 1.0 for m in range(3)]
        factors = [(1.0 + signs[m] * coords[m]) / 2.0 for m in range(3)]
        for j in range(3):
            others = [factors[m] for m in range(3) if m != j]
            contract[8 * j + vertex, :NODES] = signs[j] / 2.0 * others[0] * others[1] * quadrature
    contract[24, :NODES] = quadrature
    unit = np.eye(P_SIZE)
    directional = np.zeros((3, ROWS, NODES))
    directional[0, :NODES] = np.kron(np.kron(derivative, unit), unit)
    directional[1, :NODES] = np.kron(np.kron(unit, derivative), unit)
    directional[2, :NODES] = np.kron(np.kron(unit, unit), derivative)
    near = directional[1:]
    return (
        np.stack(halves(directional[0])),
        np.stack(halves(near[:, :HEAD, :256].reshape(2 * HEAD, 256))),
        np.stack(halves(near[:, HEAD:, BACK:].reshape(2 * TAIL, NODES - BACK))),
        np.concatenate(halves(contract)),
    )


def split(value):
    high = value.astype(BF16)
    return (high, (value - high.astype(F32)).astype(BF16))


def derivatives(fields, far, head, tail):
    high, low = split(fields)

    def apply(table, begin, end):
        return (
            jnp.dot(table[0], high[begin:end], preferred_element_type=F32)
            + jnp.dot(table[1], high[begin:end], preferred_element_type=F32)
            + jnp.dot(table[0], low[begin:end], preferred_element_type=F32)
        )

    first = apply(far, 0, NODES)
    upper = apply(head, 0, 256)
    lower = apply(tail, BACK, NODES)
    rest = [
        jnp.concatenate([upper[j * HEAD : (j + 1) * HEAD], lower[j * TAIL : (j + 1) * TAIL]], axis=0)
        for j in range(2)
    ]
    return [first, *rest]


def element_terms(grads, spacing, live, contract):
    slots = spacing.shape[1]

    def grad(field, i, j):
        column = (3 * field + i) * slots
        return grads[j][:, column : column + slots]

    def product(c, j):
        return sum(grad(0, i, c) * grad(1, i, j) for i in range(3))

    pairs = [(0, 1), (0, 2), (1, 2)]
    stack = [product(m, m) for m in range(3)]
    stack += [product(c, j) + product(j, c) for c, j in pairs]
    stack += [sum(grad(0, i, j) * grad(0, i, j) for i in range(3)) for j in range(3)]
    stack_high, stack_low = split(jnp.concatenate(stack, axis=1))
    both = jnp.dot(contract, stack_high, preferred_element_type=F32)
    sums = both[:32] + both[32:] + jnp.dot(contract[:32], stack_low, preferred_element_type=F32)

    def part(j, column):
        return sums[8 * j : 8 * j + 8, column * slots : (column + 1) * slots]

    factor = [2.0 / spacing[j : j + 1] for j in range(3)]
    square = [f * f for f in factor]
    jacobian = spacing[0:1] * spacing[1:2] * spacing[2:3] * 0.125
    terms = []
    for c in range(3):
        total = sum(square[m] * part(c, m) for m in range(3)) - 2.0 * square[c] * part(c, c)
        for column, pair in enumerate(pairs):
            if c in pair:
                j = pair[0] + pair[1] - c
                total = total - square[j] * part(j, 3 + column)
        terms.append(jnp.where(live, total * (factor[c] * jacobian), 0.0))
    spent = sum(square[j] * part(3, 6 + j) for j in range(3)) * jacobian
    return (terms, jnp.where(live, spent, 0.0))


def place(index, rows, values=None):
    slots = index.shape[1]
    row = lax.broadcasted_iota(jnp.int32, (rows, slots), 0)
    columns = []
    for k in range(8):
        hit = row == index[k : k + 1]
        if values is None:
            columns.append(jnp.where(hit, 1.0, 0.0).astype(BF16))
        else:
            columns.append(
                jnp.concatenate(
                    [jnp.where(hit, v[k : k + 1], 0.0).astype(BF16) for v in values], axis=0
                )
            )
    return jnp.concatenate(columns, axis=1)


def kernel(
    groups, columns,
    velocity_in, adjoint_in, spacing_in, count_in, map_in, far_in, head_in, tail_in, contract_in,
    direction, objective,
    velocity, adjoint, spacing, count, design_map, far, head, tail, contract,
    outgoing, maps, arrived, placed, gathered,
    local_sem, send_map, recv_map, send_sem, recv_sem, send_all, recv_all,
):
    devices = groups * columns
    grp, col = lax.axis_index("grp"), lax.axis_index("elem")
    me = grp * columns + col
    slots = spacing.shape[1]

    barrier = pltpu.get_barrier_semaphore()
    pairs = [
        (head_in, head), (velocity_in, velocity), (adjoint_in, adjoint), (far_in, far),
        (tail_in, tail), (map_in, design_map), (spacing_in, spacing), (count_in, count),
        (contract_in, contract),
    ]
    loads = [pltpu.make_async_copy(a, b, local_sem.at[i]) for i, (a, b) in enumerate(pairs)]
    for load in loads:
        load.start()

    def coords(step):
        peer = lax.rem(me + step, devices)
        return (peer // columns, lax.rem(peer, columns))

    def greet(step, carry):
        pl.semaphore_signal(barrier, inc=1, device_id=coords(step), device_id_type=MESH)
        return carry

    lax.fori_loop(1, devices, greet, 0)
    for load in loads:
        load.wait()

    fields = jnp.concatenate([f[i] for f in (velocity, adjoint) for i in range(3)], axis=1)
    grads = derivatives(fields, far[...], head[...], tail[...])

    pl.semaphore_wait(barrier, devices - 1)
    own = groups
    partners = []
    for step in [*range(groups // 2, groups), *range(groups // 2)]:
        for o in range(3):
            slot = o * groups + step
            if slot != own:
                there = (lax.rem(grp + step, groups), lax.rem(col + (o - 1 + columns), columns))
                partners.append((slot, there))

    def copies(source, target, send, receive):
        return {
            slot: pltpu.make_async_remote_copy(
                src_ref=source,
                dst_ref=target.at[slot],
                send_sem=send.at[slot],
                recv_sem=receive.at[slot],
                device_id=there,
                device_id_type=MESH,
            )
            for slot, there in partners
        }

    map_copies = copies(design_map, maps, send_map, recv_map)
    for copy in map_copies.values():
        copy.start()

    live = lax.broadcasted_iota(jnp.int32, (8, slots), 1) < count[0]
    terms, spent = element_terms(grads, spacing[...], live, contract[...])
    for c in range(3):
        outgoing[8 * c : 8 * c + 8, :] = terms[c]
    term_copies = copies(outgoing, arrived, send_sem, recv_sem)
    for copy in term_copies.values():
        copy.start()

    for slot, copy in map_copies.items():
        copy.wait()
        placed[slot] = place(maps[slot] & (LANES - 1), LANES)

    base = me * UPPER

    def collect(nodes, term, lower):
        index = lax.shift_right_logical(nodes, jnp.full_like(nodes, LANES.bit_length() - 1)) - base
        highs = [term[8 * c : 8 * c + 8].astype(BF16).astype(F32) for c in range(3)]
        lows = [term[8 * c : 8 * c + 8] - highs[c] for c in range(3)]
        return lax.dot_general(
            place(index, UPPER, highs + lows),
            lower,
            (((1,), (1,)), ((), ())),
            preferred_element_type=F32,
        )

    nodes = design_map[...]
    both = collect(nodes, outgoing[...], place(nodes & (LANES - 1), LANES))
    for slot, copy in list(term_copies.items())[::-1]:
        copy.wait_recv()
        both = both + collect(maps[slot], arrived[slot], placed[slot])
    total = both[: 3 * UPPER] + both[3 * UPPER :]

    squares = total * total
    squares = sum(squares[8 * i : 8 * i + 8] for i in range(3 * UPPER // 8))
    lane = lax.broadcasted_iota(jnp.int32, (8, LANES), 1)
    mixed = jnp.where(
        lane < LANES // 2,
        squares + pltpu.roll(squares, LANES // 2, 1),
        spent + pltpu.roll(spent, LANES // 2, 1),
    )
    gathered[me] = jnp.sum(mixed, axis=0, keepdims=True)

    def share(step):
        return pltpu.make_async_remote_copy(
            src_ref=gathered.at[me],
            dst_ref=gathered.at[me],
            send_sem=send_all.at[step],
            recv_sem=recv_all.at[step],
            device_id=coords(step),
            device_id_type=MESH,
        )

    def send(step, carry):
        share(step).start()
        return carry

    def receive(step, carry):
        share(step).wait_recv()
        return carry

    def finish(step, carry):
        share(step).wait_send()
        return carry

    lax.fori_loop(1, devices, send, 0)
    for copy in term_copies.values():
        copy.wait_send()
    lax.fori_loop(1, devices, receive, 0)
    everything = jnp.sum(gathered[...], axis=0)
    first = lax.broadcasted_iota(jnp.int32, (1, LANES), 1) < LANES // 2
    square_total = jnp.sum(jnp.where(first, everything, 0.0), axis=1, keepdims=True)
    spent_total = jnp.sum(jnp.where(first, 0.0, everything), axis=1, keepdims=True)
    scale = lax.rsqrt(square_total * (1.0 / (3.0 * ND_DEV * devices)) + 1e-06)
    scaled = total * scale
    for c in range(3):
        direction[c] = scaled[UPPER * c : UPPER * c + UPPER]
    objective[...] = spent_total * (1.0 / (NODES * slots * devices))
    lax.fori_loop(1, devices, finish, 0)


def body(groups, columns, velocity, adjoint, spacing, elem_count, design_map):
    devices = groups * columns
    blocks = 3 * groups
    slots = spacing.shape[1]
    vmem = pl.BlockSpec(memory_space=pltpu.VMEM)
    constants = tables()
    direction, objective = pl.pallas_call(
        functools.partial(kernel, groups, columns),
        out_shape=(
            jax.ShapeDtypeStruct((3, UPPER, LANES), F32),
            jax.ShapeDtypeStruct((1, 1), F32),
        ),
        in_specs=[pl.BlockSpec(memory_space=pl.ANY)] * 9,
        out_specs=(vmem, vmem),
        scratch_shapes=[
            pltpu.VMEM(velocity.shape, F32),
            pltpu.VMEM(adjoint.shape, F32),
            pltpu.VMEM(spacing.shape, F32),
            pltpu.SMEM((1,), jnp.int32),
            pltpu.VMEM((8, slots), jnp.int32),
            *[pltpu.VMEM(table.shape, BF16) for table in constants],
            pltpu.VMEM((24, slots), F32),
            pltpu.VMEM((blocks, 8, slots), jnp.int32),
            pltpu.VMEM((blocks, 24, slots), F32),
            pltpu.VMEM((blocks, LANES, 8 * slots), BF16),
            pltpu.VMEM((devices, 1, LANES), F32),
            pltpu.SemaphoreType.DMA((9,)),
            *[pltpu.SemaphoreType.DMA((blocks,))] * 4,
            *[pltpu.SemaphoreType.DMA((devices,))] * 2,
        ],
        compiler_params=pltpu.CompilerParams(collective_id=0, has_side_effects=True),
    )(velocity, adjoint, spacing, elem_count, design_map, *constants)
    return (direction.reshape(3, ND_DEV), objective.reshape(()))


def solution(mesh):
    return jax.shard_map(
        functools.partial(body, mesh.shape["grp"], mesh.shape["elem"]),
        mesh=mesh,
        in_specs=(
            P(None, None, ("grp", "elem")),
            P(None, None, ("grp", "elem")),
            P(None, ("grp", "elem")),
            P(("grp", "elem")),
            P(None, ("grp", "elem")),
        ),
        out_specs=(P(None, ("grp", "elem")), P()),
        check_vma=False,
    )
```

```python
import functools

import jax
import jax.numpy as jnp
import numpy as np
from jax import lax
from jax.experimental import pallas as pl
from jax.experimental.pallas import tpu as pltpu
from jax.sharding import PartitionSpec as P

P_SIZE = 7
ND_DEV = 2048
LANES = 128
UPPER = ND_DEV // LANES
NODES = P_SIZE**3
ROWS = -(-NODES // 16) * 16
HEAD = 240
BACK = 192
TAIL = ROWS - HEAD
MESH = pl.DeviceIdType.MESH
F32 = jnp.float32
BF16 = jnp.bfloat16


def lobatto(degree):
    points = np.cos(np.pi * np.arange(degree + 1) / degree)
    for sweep in range(60):
        lower = np.ones(degree + 1)
        upper = points.copy()
        for order in range(2, degree + 1):
            lower, upper = (upper, ((2 * order - 1) * points * upper - (order - 1) * lower) / order)
        points = points - (points * upper - lower) / ((degree + 1) * upper)
    lower = np.ones(degree + 1)
    upper = points.copy()
    for order in range(2, degree + 1):
        lower, upper = (upper, ((2 * order - 1) * points * upper - (order - 1) * lower) / order)
    return (points[::-1].copy(), upper[::-1].copy())


def halves(table):
    exact = np.asarray(table, np.float32)
    high = exact.astype(BF16)
    low = (exact - high.astype(np.float32)).astype(BF16)
    return (high, low)


def derivative_table():
    degree = P_SIZE - 1
    points, values = lobatto(degree)
    derivative = np.zeros((P_SIZE, P_SIZE))
    for i in range(P_SIZE):
        for j in range(P_SIZE):
            if i != j:
                derivative[i, j] = values[i] / (values[j] * (points[i] - points[j]))
    derivative[0, 0] = -degree * (degree + 1) / 4.0
    derivative[P_SIZE - 1, P_SIZE - 1] = degree * (degree + 1) / 4.0
    return derivative


def tables():
    degree = P_SIZE - 1
    points, values = lobatto(degree)
    weights = 2.0 / (degree * (degree + 1) * values**2)
    derivative = derivative_table()
    coords = np.meshgrid(points, points, points, indexing="ij")
    coords = [c.reshape(-1) for c in coords]
    spread = np.meshgrid(weights, weights, weights, indexing="ij")
    quadrature = (spread[0] * spread[1] * spread[2]).reshape(-1)
    contract = np.zeros((32, ROWS))
    for vertex in range(8):
        signs = [2.0 * (vertex >> 2 - m & 1) - 1.0 for m in range(3)]
        factors = [(1.0 + signs[m] * coords[m]) / 2.0 for m in range(3)]
        for j in range(3):
            others = [factors[m] for m in range(3) if m != j]
            contract[8 * j + vertex, :NODES] = signs[j] / 2.0 * others[0] * others[1] * quadrature
    contract[24, :NODES] = quadrature
    unit = np.eye(P_SIZE)
    near = np.zeros((2, ROWS, NODES))
    near[0, :NODES] = np.kron(np.kron(unit, derivative), unit)
    near[1, :NODES] = np.kron(np.kron(unit, unit), derivative)
    return (
        np.stack(halves(near[:, :HEAD, :256].reshape(2 * HEAD, 256))),
        np.stack(halves(near[:, HEAD:, BACK:].reshape(2 * TAIL, NODES - BACK))),
        np.concatenate(halves(contract)),
    )


def split(value):
    high = value.astype(BF16)
    return (high, (value - high.astype(F32)).astype(BF16))


def far_derivatives(velocity, adjoint, far):
    table = derivative_table()
    width = P_SIZE * P_SIZE
    for f, field in enumerate((velocity, adjoint)):
        for i in range(3):
            far[3 * f + i, ROWS - 16 :, :] = jnp.zeros((16, field.shape[2]), F32)
            slabs = [field[i, pl.ds(width * a, width), :] for a in range(P_SIZE)]
            for a in range(P_SIZE):
                far[3 * f + i, pl.ds(width * a, width), :] = sum(
                    float(table[a, b]) * slabs[b] for b in range(P_SIZE)
                )


def near_derivatives(fields, head, tail):
    high, low = split(fields)

    def apply(table, begin, end):
        return (
            jnp.dot(table[0], high[begin:end], preferred_element_type=F32)
            + jnp.dot(table[1], high[begin:end], preferred_element_type=F32)
            + jnp.dot(table[0], low[begin:end], preferred_element_type=F32)
        )

    upper = apply(head, 0, 256)
    lower = apply(tail, BACK, NODES)
    return [
        jnp.concatenate([upper[j * HEAD : (j + 1) * HEAD], lower[j * TAIL : (j + 1) * TAIL]], axis=0)
        for j in range(2)
    ]


def element_terms(far, near, spacing, live, contract):
    slots = spacing.shape[1]

    def grad(field, i, j):
        column = (3 * field + i) * slots
        return near[j - 1][:, column : column + slots] if j else far[3 * field + i]

    def product(c, j):
        return sum(grad(0, i, c) * grad(1, i, j) for i in range(3))

    pairs = [(0, 1), (0, 2), (1, 2)]
    stack = [product(m, m) for m in range(3)]
    stack += [product(c, j) + product(j, c) for c, j in pairs]
    stack += [sum(grad(0, i, j) * grad(0, i, j) for i in range(3)) for j in range(3)]
    stack_high, stack_low = split(jnp.concatenate(stack, axis=1))
    both = jnp.dot(contract, stack_high, preferred_element_type=F32)
    sums = both[:32] + both[32:] + jnp.dot(contract[:32], stack_low, preferred_element_type=F32)

    def part(j, column):
        return sums[8 * j : 8 * j + 8, column * slots : (column + 1) * slots]

    factor = [2.0 / spacing[j : j + 1] for j in range(3)]
    square = [f * f for f in factor]
    jacobian = spacing[0:1] * spacing[1:2] * spacing[2:3] * 0.125
    terms = []
    for c in range(3):
        total = sum(square[m] * part(c, m) for m in range(3)) - 2.0 * square[c] * part(c, c)
        for column, pair in enumerate(pairs):
            if c in pair:
                j = pair[0] + pair[1] - c
                total = total - square[j] * part(j, 3 + column)
        terms.append(jnp.where(live, total * (factor[c] * jacobian), 0.0))
    spent = sum(square[j] * part(3, 6 + j) for j in range(3)) * jacobian
    return (terms, jnp.where(live, spent, 0.0))


def place(index, rows, values=None):
    slots = index.shape[1]
    row = lax.broadcasted_iota(jnp.int32, (rows, slots), 0)
    columns = []
    for k in range(8):
        hit = row == index[k : k + 1]
        if values is None:
            columns.append(jnp.where(hit, 1.0, 0.0).astype(BF16))
        else:
            columns.append(
                jnp.concatenate(
                    [jnp.where(hit, v[k : k + 1], 0.0).astype(BF16) for v in values], axis=0
                )
            )
    return jnp.concatenate(columns, axis=1)


def kernel(
    groups, columns,
    velocity_in, adjoint_in, spacing_in, count_in, map_in, head_in, tail_in, contract_in,
    direction, objective,
    velocity, adjoint, spacing, count, design_map, head, tail, contract, far,
    outgoing, maps, arrived, placed, gathered,
    local_sem, send_map, recv_map, send_sem, recv_sem, send_all, recv_all,
):
    devices = groups * columns
    grp, col = lax.axis_index("grp"), lax.axis_index("elem")
    me = grp * columns + col
    slots = spacing.shape[1]

    barrier = pltpu.get_barrier_semaphore()
    pairs = [
        (velocity_in, velocity), (adjoint_in, adjoint), (head_in, head), (tail_in, tail),
        (map_in, design_map), (spacing_in, spacing), (count_in, count), (contract_in, contract),
    ]
    loads = [pltpu.make_async_copy(a, b, local_sem.at[i]) for i, (a, b) in enumerate(pairs)]
    for load in loads:
        load.start()

    def coords(step):
        peer = lax.rem(me + step, devices)
        return (peer // columns, lax.rem(peer, columns))

    def greet(step, carry):
        pl.semaphore_signal(barrier, inc=1, device_id=coords(step), device_id_type=MESH)
        return carry

    lax.fori_loop(1, devices, greet, 0)
    for load in loads[:4]:
        load.wait()

    fields = jnp.concatenate([f[i] for f in (velocity, adjoint) for i in range(3)], axis=1)
    near = near_derivatives(fields, head, tail)
    far_derivatives(velocity, adjoint, far)

    for load in loads[4:]:
        load.wait()
    pl.semaphore_wait(barrier, devices - 1)
    own = groups
    partners = []
    for step in [*range(groups // 2, groups), *range(groups // 2)]:
        for o in range(3):
            slot = o * groups + step
            if slot != own:
                there = (lax.rem(grp + step, groups), lax.rem(col + (o - 1 + columns), columns))
                partners.append((slot, there))

    def copies(source, target, send, receive):
        return {
            slot: pltpu.make_async_remote_copy(
                src_ref=source,
                dst_ref=target.at[slot],
                send_sem=send.at[slot],
                recv_sem=receive.at[slot],
                device_id=there,
                device_id_type=MESH,
            )
            for slot, there in partners
        }

    map_copies = copies(design_map, maps, send_map, recv_map)
    for copy in map_copies.values():
        copy.start()

    live = lax.broadcasted_iota(jnp.int32, (8, slots), 1) < count[0]
    terms, spent = element_terms(far, near, spacing[...], live, contract[...])
    for c in range(3):
        outgoing[8 * c : 8 * c + 8, :] = terms[c]
    term_copies = copies(outgoing, arrived, send_sem, recv_sem)
    for copy in term_copies.values():
        copy.start()

    base = me * UPPER

    def collect(nodes, term, lower):
        index = lax.shift_right_logical(nodes, jnp.full_like(nodes, LANES.bit_length() - 1)) - base
        highs = [term[8 * c : 8 * c + 8].astype(BF16).astype(F32) for c in range(3)]
        lows = [term[8 * c : 8 * c + 8] - highs[c] for c in range(3)]
        return lax.dot_general(
            place(index, UPPER, highs + lows),
            lower,
            (((1,), (1,)), ((), ())),
            preferred_element_type=F32,
        )

    nodes = design_map[...]
    both = collect(nodes, outgoing[...], place(nodes & (LANES - 1), LANES))
    for slot, copy in map_copies.items():
        copy.wait()
        placed[slot] = place(maps[slot] & (LANES - 1), LANES)

    for slot, copy in list(term_copies.items())[::-1]:
        copy.wait_recv()
        both = both + collect(maps[slot], arrived[slot], placed[slot])
    total = both[: 3 * UPPER] + both[3 * UPPER :]

    squares = total * total
    squares = sum(squares[8 * i : 8 * i + 8] for i in range(3 * UPPER // 8))
    lane = lax.broadcasted_iota(jnp.int32, (8, LANES), 1)
    mixed = jnp.where(
        lane < LANES // 2,
        squares + pltpu.roll(squares, LANES // 2, 1),
        spent + pltpu.roll(spent, LANES // 2, 1),
    )
    gathered[me] = jnp.sum(mixed, axis=0, keepdims=True)

    def share(step):
        return pltpu.make_async_remote_copy(
            src_ref=gathered.at[me],
            dst_ref=gathered.at[me],
            send_sem=send_all.at[step],
            recv_sem=recv_all.at[step],
            device_id=coords(step),
            device_id_type=MESH,
        )

    def send(step, carry):
        share(step).start()
        return carry

    def receive(step, carry):
        share(step).wait_recv()
        return carry

    def finish(step, carry):
        share(step).wait_send()
        return carry

    lax.fori_loop(1, devices, send, 0)
    for copy in term_copies.values():
        copy.wait_send()
    lax.fori_loop(1, devices, receive, 0)
    everything = jnp.sum(gathered[...], axis=0)
    first = lax.broadcasted_iota(jnp.int32, (1, LANES), 1) < LANES // 2
    square_total = jnp.sum(jnp.where(first, everything, 0.0), axis=1, keepdims=True)
    spent_total = jnp.sum(jnp.where(first, 0.0, everything), axis=1, keepdims=True)
    scale = lax.rsqrt(square_total * (1.0 / (3.0 * ND_DEV * devices)) + 1e-06)
    scaled = total * scale
    for c in range(3):
        direction[c] = scaled[UPPER * c : UPPER * c + UPPER]
    objective[...] = spent_total * (1.0 / (NODES * slots * devices))
    lax.fori_loop(1, devices, finish, 0)


def body(groups, columns, velocity, adjoint, spacing, elem_count, design_map):
    devices = groups * columns
    blocks = 3 * groups
    slots = spacing.shape[1]
    vmem = pl.BlockSpec(memory_space=pltpu.VMEM)
    constants = tables()
    direction, objective = pl.pallas_call(
        functools.partial(kernel, groups, columns),
        out_shape=(
            jax.ShapeDtypeStruct((3, UPPER, LANES), F32),
            jax.ShapeDtypeStruct((1, 1), F32),
        ),
        in_specs=[pl.BlockSpec(memory_space=pl.ANY)] * 8,
        out_specs=(vmem, vmem),
        scratch_shapes=[
            pltpu.VMEM(velocity.shape, F32),
            pltpu.VMEM(adjoint.shape, F32),
            pltpu.VMEM(spacing.shape, F32),
            pltpu.SMEM((1,), jnp.int32),
            pltpu.VMEM((8, slots), jnp.int32),
            *[pltpu.VMEM(table.shape, BF16) for table in constants],
            pltpu.VMEM((6, ROWS, slots), F32),
            pltpu.VMEM((24, slots), F32),
            pltpu.VMEM((blocks, 8, slots), jnp.int32),
            pltpu.VMEM((blocks, 24, slots), F32),
            pltpu.VMEM((blocks, LANES, 8 * slots), BF16),
            pltpu.VMEM((devices, 1, LANES), F32),
            pltpu.SemaphoreType.DMA((8,)),
            *[pltpu.SemaphoreType.DMA((blocks,))] * 4,
            *[pltpu.SemaphoreType.DMA((devices,))] * 2,
        ],
        compiler_params=pltpu.CompilerParams(collective_id=0, has_side_effects=True),
    )(velocity, adjoint, spacing, elem_count, design_map, *constants)
    return (direction.reshape(3, ND_DEV), objective.reshape(()))


def solution(mesh):
    return jax.shard_map(
        functools.partial(body, mesh.shape["grp"], mesh.shape["elem"]),
        mesh=mesh,
        in_specs=(
            P(None, None, ("grp", "elem")),
            P(None, None, ("grp", "elem")),
            P(None, ("grp", "elem")),
            P(("grp", "elem")),
            P(None, ("grp", "elem")),
        ),
        out_specs=(P(None, ("grp", "elem")), P()),
        check_vma=False,
    )
```

```python
import functools

import jax
import jax.numpy as jnp
import numpy as np
from jax import lax
from jax.experimental import pallas as pl
from jax.experimental.pallas import tpu as pltpu
from jax.sharding import PartitionSpec as P

P_SIZE = 7
ND_DEV = 2048
LANES = 128
UPPER = ND_DEV // LANES
NODES = P_SIZE**3
ROWS = -(-NODES // 16) * 16
HEAD = 240
BACK = 192
TAIL = ROWS - HEAD
MESH = pl.DeviceIdType.MESH
F32 = jnp.float32
BF16 = jnp.bfloat16


def lobatto(degree):
    points = np.cos(np.pi * np.arange(degree + 1) / degree)
    for sweep in range(60):
        lower = np.ones(degree + 1)
        upper = points.copy()
        for order in range(2, degree + 1):
            lower, upper = (upper, ((2 * order - 1) * points * upper - (order - 1) * lower) / order)
        points = points - (points * upper - lower) / ((degree + 1) * upper)
    lower = np.ones(degree + 1)
    upper = points.copy()
    for order in range(2, degree + 1):
        lower, upper = (upper, ((2 * order - 1) * points * upper - (order - 1) * lower) / order)
    return (points[::-1].copy(), upper[::-1].copy())


def halves(table):
    exact = np.asarray(table, np.float32)
    high = exact.astype(BF16)
    low = (exact - high.astype(np.float32)).astype(BF16)
    return (high, low)


def derivative_table():
    degree = P_SIZE - 1
    points, values = lobatto(degree)
    derivative = np.zeros((P_SIZE, P_SIZE))
    for i in range(P_SIZE):
        for j in range(P_SIZE):
            if i != j:
                derivative[i, j] = values[i] / (values[j] * (points[i] - points[j]))
    derivative[0, 0] = -degree * (degree + 1) / 4.0
    derivative[P_SIZE - 1, P_SIZE - 1] = degree * (degree + 1) / 4.0
    return derivative


def tables():
    degree = P_SIZE - 1
    points, values = lobatto(degree)
    weights = 2.0 / (degree * (degree + 1) * values**2)
    derivative = derivative_table()
    coords = np.meshgrid(points, points, points, indexing="ij")
    coords = [c.reshape(-1) for c in coords]
    spread = np.meshgrid(weights, weights, weights, indexing="ij")
    quadrature = (spread[0] * spread[1] * spread[2]).reshape(-1)
    contract = np.zeros((32, ROWS))
    for vertex in range(8):
        signs = [2.0 * (vertex >> 2 - m & 1) - 1.0 for m in range(3)]
        factors = [(1.0 + signs[m] * coords[m]) / 2.0 for m in range(3)]
        for j in range(3):
            others = [factors[m] for m in range(3) if m != j]
            contract[8 * j + vertex, :NODES] = signs[j] / 2.0 * others[0] * others[1] * quadrature
    contract[24, :NODES] = quadrature
    unit = np.eye(P_SIZE)
    near = np.zeros((2, ROWS, NODES))
    near[0, :NODES] = np.kron(np.kron(unit, derivative), unit)
    near[1, :NODES] = np.kron(np.kron(unit, unit), derivative)
    return (
        np.stack(halves(near[:, :HEAD, :256].reshape(2 * HEAD, 256))),
        np.stack(halves(near[:, HEAD:, BACK:].reshape(2 * TAIL, NODES - BACK))),
        np.concatenate(halves(contract)),
    )


def split(value):
    high = value.astype(BF16)
    return (high, (value - high.astype(F32)).astype(BF16))


def far_derivatives(velocity, adjoint, far):
    table = derivative_table()
    width = P_SIZE * P_SIZE
    for f, field in enumerate((velocity, adjoint)):
        for i in range(3):
            far[3 * f + i, ROWS - 16 :, :] = jnp.zeros((16, field.shape[2]), F32)
            slabs = [field[i, pl.ds(width * a, width), :] for a in range(P_SIZE)]
            for a in range(P_SIZE):
                far[3 * f + i, pl.ds(width * a, width), :] = sum(
                    float(table[a, b]) * slabs[b] for b in range(P_SIZE)
                )


def near_derivatives(fields, head, tail):
    high, low = split(fields)

    def apply(table, begin, end):
        return (
            jnp.dot(table[0], high[begin:end], preferred_element_type=F32)
            + jnp.dot(table[1], high[begin:end], preferred_element_type=F32)
            + jnp.dot(table[0], low[begin:end], preferred_element_type=F32)
        )

    upper = apply(head, 0, 256)
    lower = apply(tail, BACK, NODES)
    return [
        jnp.concatenate([upper[j * HEAD : (j + 1) * HEAD], lower[j * TAIL : (j + 1) * TAIL]], axis=0)
        for j in range(2)
    ]


def element_terms(far, near, spacing, live, contract):
    slots = spacing.shape[1]

    def grad(field, i, j):
        column = (3 * field + i) * slots
        return near[j - 1][:, column : column + slots] if j else far[3 * field + i]

    def product(c, j):
        return sum(grad(0, i, c) * grad(1, i, j) for i in range(3))

    pairs = [(0, 1), (0, 2), (1, 2)]
    stack = [product(m, m) for m in range(3)]
    stack += [product(c, j) + product(j, c) for c, j in pairs]
    stack += [sum(grad(0, i, j) * grad(0, i, j) for i in range(3)) for j in range(3)]
    stack_high, stack_low = split(jnp.concatenate(stack, axis=1))
    both = jnp.dot(contract, stack_high, preferred_element_type=F32)
    sums = both[:32] + both[32:] + jnp.dot(contract[:32], stack_low, preferred_element_type=F32)

    def part(j, column):
        return sums[8 * j : 8 * j + 8, column * slots : (column + 1) * slots]

    factor = [2.0 / spacing[j : j + 1] for j in range(3)]
    square = [f * f for f in factor]
    jacobian = spacing[0:1] * spacing[1:2] * spacing[2:3] * 0.125
    terms = []
    for c in range(3):
        total = sum(square[m] * part(c, m) for m in range(3)) - 2.0 * square[c] * part(c, c)
        for column, pair in enumerate(pairs):
            if c in pair:
                j = pair[0] + pair[1] - c
                total = total - square[j] * part(j, 3 + column)
        terms.append(jnp.where(live, total * (factor[c] * jacobian), 0.0))
    spent = sum(square[j] * part(3, 6 + j) for j in range(3)) * jacobian
    return (terms, jnp.where(live, spent, 0.0))


def place(index, rows, values=None):
    slots = index.shape[1]
    row = lax.broadcasted_iota(jnp.int32, (rows, slots), 0)
    columns = []
    for k in range(8):
        hit = row == index[k : k + 1]
        if values is None:
            columns.append(jnp.where(hit, 1.0, 0.0).astype(BF16))
        else:
            columns.append(
                jnp.concatenate(
                    [jnp.where(hit, v[k : k + 1], 0.0).astype(BF16) for v in values], axis=0
                )
            )
    return jnp.concatenate(columns, axis=1)


def kernel(
    groups, columns,
    velocity_in, adjoint_in, spacing_in, count_in, map_in, head_in, tail_in, contract_in,
    direction, objective,
    velocity, adjoint, spacing, count, design_map, head, tail, contract, far,
    outgoing, maps, arrived, placed, gathered,
    local_sem, send_map, recv_map, send_sem, recv_sem, send_all, recv_all,
):
    devices = groups * columns
    grp, col = lax.axis_index("grp"), lax.axis_index("elem")
    me = grp * columns + col
    slots = spacing.shape[1]

    barrier = pltpu.get_barrier_semaphore()
    pairs = [
        (velocity_in, velocity), (adjoint_in, adjoint), (head_in, head), (tail_in, tail),
        (map_in, design_map), (spacing_in, spacing), (count_in, count), (contract_in, contract),
    ]
    loads = [pltpu.make_async_copy(a, b, local_sem.at[i]) for i, (a, b) in enumerate(pairs)]
    for load in loads:
        load.start()

    def coords(step):
        peer = lax.rem(me + step, devices)
        return (peer // columns, lax.rem(peer, columns))

    def greet(step, carry):
        pl.semaphore_signal(barrier, inc=1, device_id=coords(step), device_id_type=MESH)
        return carry

    lax.fori_loop(1, devices, greet, 0)
    for load in loads[:4]:
        load.wait()

    fields = jnp.concatenate([f[i] for f in (velocity, adjoint) for i in range(3)], axis=1)
    near = near_derivatives(fields, head, tail)
    far_derivatives(velocity, adjoint, far)

    for load in loads[4:]:
        load.wait()
    own = groups
    partners = []
    for step in [*range(groups // 2, groups), *range(groups // 2)]:
        for o in range(3):
            slot = o * groups + step
            if slot != own:
                there = (lax.rem(grp + step, groups), lax.rem(col + (o - 1 + columns), columns))
                partners.append((slot, there))

    def copies(source, target, send, receive):
        return {
            slot: pltpu.make_async_remote_copy(
                src_ref=source,
                dst_ref=target.at[slot],
                send_sem=send.at[slot],
                recv_sem=receive.at[slot],
                device_id=there,
                device_id_type=MESH,
            )
            for slot, there in partners
        }

    map_copies = copies(design_map, maps, send_map, recv_map)

    live = lax.broadcasted_iota(jnp.int32, (8, slots), 1) < count[0]
    terms, spent = element_terms(far, near, spacing[...], live, contract[...])
    for c in range(3):
        outgoing[8 * c : 8 * c + 8, :] = terms[c]
    term_copies = copies(outgoing, arrived, send_sem, recv_sem)
    pl.semaphore_wait(barrier, devices - 1)
    for copy in map_copies.values():
        copy.start()
    for copy in term_copies.values():
        copy.start()

    base = me * UPPER

    def collect(nodes, term, lower):
        index = lax.shift_right_logical(nodes, jnp.full_like(nodes, LANES.bit_length() - 1)) - base
        highs = [term[8 * c : 8 * c + 8].astype(BF16).astype(F32) for c in range(3)]
        lows = [term[8 * c : 8 * c + 8] - highs[c] for c in range(3)]
        return lax.dot_general(
            place(index, UPPER, highs + lows),
            lower,
            (((1,), (1,)), ((), ())),
            preferred_element_type=F32,
        )

    nodes = design_map[...]
    both = collect(nodes, outgoing[...], place(nodes & (LANES - 1), LANES))
    for slot, copy in map_copies.items():
        copy.wait()
        placed[slot] = place(maps[slot] & (LANES - 1), LANES)

    for slot, copy in list(term_copies.items())[::-1]:
        copy.wait_recv()
        both = both + collect(maps[slot], arrived[slot], placed[slot])
    total = both[: 3 * UPPER] + both[3 * UPPER :]

    squares = total * total
    squares = sum(squares[8 * i : 8 * i + 8] for i in range(3 * UPPER // 8))
    lane = lax.broadcasted_iota(jnp.int32, (8, LANES), 1)
    mixed = jnp.where(
        lane < LANES // 2,
        squares + pltpu.roll(squares, LANES // 2, 1),
        spent + pltpu.roll(spent, LANES // 2, 1),
    )
    gathered[me] = jnp.sum(mixed, axis=0, keepdims=True)

    def share(step):
        return pltpu.make_async_remote_copy(
            src_ref=gathered.at[me],
            dst_ref=gathered.at[me],
            send_sem=send_all.at[step],
            recv_sem=recv_all.at[step],
            device_id=coords(step),
            device_id_type=MESH,
        )

    def send(step, carry):
        share(step).start()
        return carry

    def receive(step, carry):
        share(step).wait_recv()
        return carry

    def finish(step, carry):
        share(step).wait_send()
        return carry

    lax.fori_loop(1, devices, send, 0)
    for copy in term_copies.values():
        copy.wait_send()
    lax.fori_loop(1, devices, receive, 0)
    everything = jnp.sum(gathered[...], axis=0)
    first = lax.broadcasted_iota(jnp.int32, (1, LANES), 1) < LANES // 2
    square_total = jnp.sum(jnp.where(first, everything, 0.0), axis=1, keepdims=True)
    spent_total = jnp.sum(jnp.where(first, 0.0, everything), axis=1, keepdims=True)
    scale = lax.rsqrt(square_total * (1.0 / (3.0 * ND_DEV * devices)) + 1e-06)
    scaled = total * scale
    for c in range(3):
        direction[c] = scaled[UPPER * c : UPPER * c + UPPER]
    objective[...] = spent_total * (1.0 / (NODES * slots * devices))
    lax.fori_loop(1, devices, finish, 0)


def body(groups, columns, velocity, adjoint, spacing, elem_count, design_map):
    devices = groups * columns
    blocks = 3 * groups
    slots = spacing.shape[1]
    vmem = pl.BlockSpec(memory_space=pltpu.VMEM)
    constants = tables()
    direction, objective = pl.pallas_call(
        functools.partial(kernel, groups, columns),
        out_shape=(
            jax.ShapeDtypeStruct((3, UPPER, LANES), F32),
            jax.ShapeDtypeStruct((1, 1), F32),
        ),
        in_specs=[pl.BlockSpec(memory_space=pl.ANY)] * 8,
        out_specs=(vmem, vmem),
        scratch_shapes=[
            pltpu.VMEM(velocity.shape, F32),
            pltpu.VMEM(adjoint.shape, F32),
            pltpu.VMEM(spacing.shape, F32),
            pltpu.SMEM((1,), jnp.int32),
            pltpu.VMEM((8, slots), jnp.int32),
            *[pltpu.VMEM(table.shape, BF16) for table in constants],
            pltpu.VMEM((6, ROWS, slots), F32),
            pltpu.VMEM((24, slots), F32),
            pltpu.VMEM((blocks, 8, slots), jnp.int32),
            pltpu.VMEM((blocks, 24, slots), F32),
            pltpu.VMEM((blocks, LANES, 8 * slots), BF16),
            pltpu.VMEM((devices, 1, LANES), F32),
            pltpu.SemaphoreType.DMA((8,)),
            *[pltpu.SemaphoreType.DMA((blocks,))] * 4,
            *[pltpu.SemaphoreType.DMA((devices,))] * 2,
        ],
        compiler_params=pltpu.CompilerParams(collective_id=0, has_side_effects=True),
    )(velocity, adjoint, spacing, elem_count, design_map, *constants)
    return (direction.reshape(3, ND_DEV), objective.reshape(()))


def solution(mesh):
    return jax.shard_map(
        functools.partial(body, mesh.shape["grp"], mesh.shape["elem"]),
        mesh=mesh,
        in_specs=(
            P(None, None, ("grp", "elem")),
            P(None, None, ("grp", "elem")),
            P(None, ("grp", "elem")),
            P(("grp", "elem")),
            P(None, ("grp", "elem")),
        ),
        out_specs=(P(None, ("grp", "elem")), P()),
        check_vma=False,
    )
```
